256 devices in a mesh: vocab: 32 (over y, z), batch: 8 (over x, core).
Axes of the slice: x: 4, y: 4, z: 8, core: 2. Of those that a mesh axis runs over, the one named last changes fastest.
Arguments:
- tokens: bfloat16 [2048, 5120], P('batch'), may hold values from -180 to 180
- cluster_ids: int32 [2048, 1], P('batch'), may hold values from 0 to 3; in each aligned block of 256 rows (0 to 255, 256 to 511, ...) at most 128 rows name the same one
- head_weight: bfloat16 [5120, 16384], P('batch', 'vocab'), may hold values from -0.078125 to 0.078125
- cluster_weight: bfloat16 [5120, 4], replicated, may hold values from -0.078125 to 0.078125
- tail_proj: bfloat16 [5120, 2400], P('vocab'), may hold values from -0.078125 to 0.078125
- out_one: bfloat16 [1280, 16384], P(None, 'vocab'), may hold values from -0.15625 to 0.15625
- out_two: bfloat16 [640, 32768], P(None, 'vocab'), may hold values from -0.25 to 0.25
- out_three: bfloat16 [320, 32768], P(None, 'vocab'), may hold values from -0.3125 to 0.3125
- out_four: bfloat16 [160, 32768], P(None, 'vocab'), may hold values from -0.5 to 0.5
Outputs:
- head_logp: float32 [2048, 16384], P('batch', 'vocab')
- tail_one: float32 [1024, 16384], P('batch', 'vocab')
- tail_two: float32 [1024, 32768], P('batch', 'vocab')
- tail_three: float32 [1024, 32768], P('batch', 'vocab')
- tail_four: float32 [1024, 32768], P('batch', 'vocab')
The draws below stay inside these ranges and needn't reach their ends.
Inputs may be any that keep to these rules, and one draw needn't show every extreme that they name: `cluster_ids`: in the 256 rows of one index of batch no cluster is named by more than 128 rows.
All inputs are finite; a program needn't handle non-finite values.
Results may differ from the reference program's by a relative error of at most 0.00057.
Values may be sent and summed in bfloat16 or wider, within the bound.
A program may use at most 64 MiB of HBM per device.

```python
import math
import jax
import jax.numpy as jnp
import numpy as np
from jax import lax

D = 5120
CLUSTERS = 4
P1 = 1280
P2 = 640
P3 = 320
P4 = 160
SEQ_DEV = 256
CAP = 128
SEQS = 2048
HEAD = 16384
V1 = 16384
V2 = 32768
V3 = 32768
V4 = 32768
PSUM = 2400
N_BATCH = 8


def draw_tokens(key, part):
    scale_key = jax.random.fold_in(key, 11)
    value_key = jax.random.fold_in(key, 12)
    scales = jnp.exp(jax.random.uniform(scale_key, (SEQS, 1), jnp.float32, jnp.log(3.0), jnp.log(30.0)))
    values = jnp.clip(jax.random.normal(value_key, (SEQS, D), jnp.float32), -6.0, 6.0)
    return (values * scales).astype(jnp.bfloat16)


def level_of(stream_key, dims, pieces, least, top_value):
    level, own = 1.0, jax.random.fold_in(stream_key, 6)
    for axis_at, blocks in pieces:
        draws = jnp.exp(jax.random.uniform(jax.random.fold_in(own, axis_at), (blocks,), jnp.float32, least / len(pieces), top_value / len(pieces)))
        level = level * jnp.repeat(draws, dims[axis_at] // blocks).reshape([-1 if axis == axis_at else 1 for axis in range(len(dims))])
    return level


def assign_block(key, own, number, rows, amount, top, bound, lean):
    ranking = jax.random.permutation(key, amount)
    packed, common = shares(amount, rows * top, bound, lean, True), shares(amount, rows * top, bound, lean, False)
    places = jnp.arange(amount)

    def named(tallies, rotation):
        used = int((tallies > 0).sum())
        fixed = max(1, used // 4)
        passed = fixed + (places - fixed + rotation * (used - fixed)) % max(1, amount - fixed)
        return jnp.zeros((amount,), jnp.int32).at[ranking[jnp.where(places < fixed, places, passed)]].set(jnp.asarray(tallies, jnp.int32))

    tallies = jnp.where(number % 4 == 0, named(packed, number // 4), named(common, number - number // 4 - 1))
    mixed = jax.random.permutation(jax.random.fold_in(own, 3), amount)
    giver, taker = mixed[0:amount // 2 * 2:2], mixed[1:amount // 2 * 2:2]
    slack = jnp.minimum(tallies[giver] - 1, bound - tallies[taker]) // 2
    slack = jnp.where((giver == ranking[0]) | (taker == ranking[0]) | (tallies[taker] == 0), 0, jnp.maximum(slack, 0))
    passed = jax.random.randint(jax.random.fold_in(own, 4), (amount // 2,), 0, 1 << 20) % (slack + 1)
    tallies = tallies.at[giver].add(-passed).at[taker].add(passed)
    items = jnp.searchsorted(jnp.cumsum(tallies), jnp.arange(rows * top), side="right").astype(jnp.int32)
    grid = items.reshape(top, rows).T
    grid = grid[jax.random.permutation(jax.random.fold_in(own, 1), rows)]
    rotation = jax.random.randint(jax.random.fold_in(own, 2), (rows, 1), 0, top)
    return jnp.take_along_axis(grid, (jnp.arange(top)[None, :] + rotation) % top, axis=1)


def shares(amount, total, bound, lean, full):
    loads = [(1 << 20) // math.isqrt(grade ** lean) + 1 for grade in range(1, amount + 1)]
    largest = bound if full else min(bound, max(-(-total // amount), total * loads[0] // sum(loads)))
    least = 1 if total - largest >= amount - 1 else 0
    counts, surplus = [largest] + [least] * (amount - 1), total - largest - least * (amount - 1)
    while surplus > 0:
        free = [i for i in range(1, amount) if counts[i] < largest] or [i for i in range(1, amount) if counts[i] < bound]
        mass, budget = sum([loads[i] for i in free]), surplus
        for i in free:
            extra = min(bound - counts[i], max(1, budget * loads[i] // mass), surplus)
            counts[i] = counts[i] + extra
            surplus = surplus - extra
    return np.array(counts)


def gaussian(stream_key, shape, scale, most, shards=(), kind=jnp.bfloat16):
    level = level_of(stream_key, shape, shards, -0.22, 0.18) if shards else 1.0
    values = jax.random.normal(stream_key, shape, jnp.float32) * scale * level
    return jnp.minimum(jnp.maximum(values, -most), most).astype(kind)


def setup_inputs(seed: int = 0) -> dict:
    key_list = jax.random.split(jax.random.key(seed), 10)
    tokens = draw_tokens(jax.random.fold_in(key_list[9], 71), 0)
    cluster_ids_keys = jax.random.split(jax.random.fold_in(key_list[1], 1), SEQS // SEQ_DEV)
    cluster_ids_turns = jax.random.permutation(jax.random.fold_in(key_list[1], 3), SEQS // SEQ_DEV)
    cluster_ids = jax.vmap(lambda own, number: assign_block(jax.random.fold_in(key_list[1], 2), own, number, SEQ_DEV, CLUSTERS, 1, CAP, 2))(cluster_ids_keys, cluster_ids_turns).reshape((SEQS, 1))
    head_weight = gaussian(key_list[2], (D, HEAD), D ** -0.5, 0.078125, ((0, 8), (1, 32)))
    cluster_weight = gaussian(key_list[3], (D, CLUSTERS), D ** -0.5, 0.078125)
    tail_proj = gaussian(key_list[4], (D, PSUM), D ** -0.5, 0.078125, ((0, 32),))
    out_one = gaussian(key_list[5], (P1, V1), P1 ** -0.5, 0.15625, ((1, 32),))
    out_two = gaussian(key_list[6], (P2, V2), P2 ** -0.5, 0.25, ((1, 32),))
    out_three = gaussian(key_list[7], (P3, V3), P3 ** -0.5, 0.3125, ((1, 32),))
    out_four = gaussian(key_list[8], (P4, V4), P4 ** -0.5, 0.5, ((1, 32),))
    return {"tokens": tokens, "cluster_ids": cluster_ids, "head_weight": head_weight, "cluster_weight": cluster_weight, "tail_proj": tail_proj, "out_one": out_one, "out_two": out_two, "out_three": out_three, "out_four": out_four}


def log_rows(logits):
    highest = jnp.max(logits, axis=-1, keepdims=True)
    return highest + jnp.log(jnp.sum(jnp.exp(logits - highest), axis=-1, keepdims=True))


def reference(tokens, cluster_ids, head_weight, cluster_weight, tail_proj, out_one, out_two, out_three, out_four):
    hidden = tokens.astype(jnp.float32)
    head_logits = jnp.dot(hidden, head_weight.astype(jnp.float32), precision=lax.Precision.HIGHEST)
    cluster_logits = jnp.dot(hidden, cluster_weight.astype(jnp.float32), precision=lax.Precision.HIGHEST)
    joined = jnp.concatenate([head_logits, cluster_logits], axis=1)
    log_total = log_rows(joined)
    head_logp = head_logits - log_total
    cluster_logp = cluster_logits - log_total
    cluster_of = cluster_ids[:, 0].reshape(N_BATCH, SEQ_DEV)
    labels = jnp.arange(CLUSTERS, dtype=jnp.int32)
    onehot = (cluster_of[:, :, None] == labels[None, None, :]).astype(jnp.int32)
    before = jnp.cumsum(onehot, axis=1) - onehot
    slot_of = jnp.sum(before * onehot, axis=2)
    slot_numbers = jnp.arange(CAP, dtype=jnp.int32)
    picker = ((cluster_of[:, None, None, :] == labels[None, :, None, None])
              & (slot_of[:, None, None, :] == slot_numbers[None, None, :, None])).astype(jnp.float32)
    grouped = hidden.reshape(N_BATCH, SEQ_DEV, D)
    blocks = jnp.einsum("gcjs,gsd->gcjd", picker, grouped, precision=lax.Precision.HIGHEST)
    slot_logp = jnp.einsum("gcjs,gsc->gcj", picker, cluster_logp.reshape(N_BATCH, SEQ_DEV, CLUSTERS),
                           precision=lax.Precision.HIGHEST)
    occupied = jnp.sum(picker, axis=3)
    out_weights = (out_one, out_two, out_three, out_four)
    results = []
    offset = 0
    for cluster in range(CLUSTERS):
        proj_width = out_weights[cluster].shape[0]
        block_rows = blocks[:, cluster].reshape(N_BATCH * CAP, D)
        projected = jnp.dot(block_rows, tail_proj[:, offset:offset + proj_width].astype(jnp.float32),
                            precision=lax.Precision.HIGHEST).astype(jnp.bfloat16)
        projected = lax.optimization_barrier(projected)
        offset = offset + proj_width
        logits = jnp.dot(projected.astype(jnp.float32), out_weights[cluster].astype(jnp.float32),
                         precision=lax.Precision.HIGHEST)
        scored = logits - log_rows(logits) + slot_logp[:, cluster].reshape(-1)[:, None]
        results.append(jnp.where(occupied[:, cluster].reshape(-1)[:, None] > 0, scored, jnp.zeros_like(scored)))
    return head_logp, results[0], results[1], results[2], results[3]
```

```python
import jax
import jax.numpy as jnp
from jax import lax
from jax.experimental import pallas as pl
from jax.experimental.pallas import tpu as pltpu
from jax.sharding import PartitionSpec as P

NY, NZ, NX = 4, 8, 4
NV = NY * NZ
NB = 2 * NX
TILES = 19
F32, BF16 = jnp.float32, jnp.bfloat16


def ring_place(i, y):
    return lax.rem((i * 8) // 5 + 2 * y, NZ)


def remote(src, dst, send_sem, recv_sem, v, b):
    return pltpu.make_async_remote_copy(
        src_ref=src,
        dst_ref=dst,
        send_sem=send_sem,
        recv_sem=recv_sem,
        device_id=(v, b),
        device_id_type=pl.DeviceIdType.MESH,
    )


def arrived(ref, sem):
    pltpu.make_async_copy(ref, ref, sem).wait()


def log_sum(x):
    top = jnp.max(x, axis=1, keepdims=True)
    return top + jnp.log(jnp.sum(jnp.exp(x - top), axis=1, keepdims=True))


def work(
    tok_h, ids_h, w_h, cw_h, t_h, o1_h, o2_h, o3_h, o4_h,
    head_o, s1_o, s2_o, s3_o, s4_o, off_o,
    tok, ids, wbuf, cw, tin, tv, town, pbuf, o1, o2, o3, o4, msg, xbuf, pick, rows,
    ld_w, ld_tok, ld_misc,
    wss, wrs, tss, trs, tpss, tprs, pzss, pzrs, pyss, pyrs, poss, pors, xss, xrs,
):
    v, b = lax.axis_index("vocab"), lax.axis_index("batch")
    y, z = v // NZ, lax.rem(v, NZ)
    x, c = b // 2, lax.rem(b, 2)
    right = lax.rem(x + 1, NX) * 2 + c
    left = lax.rem(x + 3, NX) * 2 + c
    far = lax.rem(x + 2, NX) * 2 + c
    mate = x * 2 + 1 - c
    y_up, y_down, y_far = lax.rem(y + 1, NY), lax.rem(y + 3, NY), lax.rem(y + 2, NY)

    load_t = pltpu.make_async_copy(t_h, tin, ld_misc.at[0])
    load_t.start()
    load_w = [
        pltpu.make_async_copy(w_h.at[:, pl.ds(128 * q, 128)], wbuf.at[b, q], ld_w.at[q])
        for q in range(4)
    ]
    for copy in load_w:
        copy.start()
    load_ids = pltpu.make_async_copy(ids_h, ids, ld_misc.at[1])
    load_ids.start()
    load_cw = pltpu.make_async_copy(cw_h, cw, ld_misc.at[2])
    load_cw.start()
    load_tok = [
        pltpu.make_async_copy(tok_h.at[:, pl.ds(640 * k, 640)], tok.at[k], ld_tok.at[k])
        for k in range(8)
    ]
    for copy in load_tok:
        copy.start()
    load_out = [
        pltpu.make_async_copy(src, dst, ld_misc.at[3 + k])
        for k, (src, dst) in enumerate(((o1_h, o1), (o2_h, o2), (o3_h, o3), (o4_h, o4)))
    ]
    for copy in load_out:
        copy.start()

    barrier = pltpu.get_barrier_semaphore()
    for peer in (right, left, mate):
        pl.semaphore_signal(barrier, inc=1, device_id=(v, peer), device_id_type=pl.DeviceIdType.MESH)

    @pl.loop(1, NV)
    def _(k):
        pl.semaphore_signal(
            barrier, inc=1, device_id=(lax.rem(v + k, NV), b), device_id_type=pl.DeviceIdType.MESH
        )

    load_t.wait()
    for j in range(TILES - 1):
        for h in range(2):
            tv[j, h] = tin[80 * h : 80 * h + 80, 128 * j : 128 * j + 128]
    for h in range(2):
        tv[TILES - 1, h] = jnp.concatenate(
            [tin[80 * h : 80 * h + 80, 2304:2400], jnp.zeros((80, 32), BF16)], axis=1
        )
    for copy in load_w:
        copy.wait()
    pl.semaphore_wait(barrier, 3 + NV - 1)

    def w_send(shard, q, to, k):
        return remote(wbuf.at[shard, q], wbuf.at[shard, q], wss.at[k], wrs.at[shard, q], v, to)

    pending = []

    def start(copy):
        copy.start()
        pending.append(copy)

    for k in range(4):
        start(w_send(b, k, right, k))
        start(w_send(b, (k + 2) % 4, left, 4 + k))
    for k in range(4):
        start(w_send(b, k, mate, 8 + k))

    def t_send(j):
        y_to = j // 5
        v_to = y_to * NZ + ring_place(lax.rem(j, 5), y_to)
        return v_to, remote(tv.at[j, c], town.at[v, c], tss.at[j], trs.at[v], v_to, b)

    @pl.loop(0, TILES)
    def _(jj):
        v_to, copy = t_send(lax.rem(jj + v, TILES))

        @pl.when(v_to != v)
        def _():
            copy.start()

    mine_r = lax.rem(z - 2 * y + 8, NZ)
    mine_i = (5 * mine_r + 7) // 8
    mine_j = 5 * y + mine_i
    owner = jnp.logical_and((mine_i * 8) // 5 == mine_r, mine_j < TILES)

    load_ids.wait()
    id_row = ids[...]
    kinds = lax.broadcasted_iota(jnp.int32, (8, 256), 0)
    onehot = jnp.where(kinds == id_row, 1.0, 0.0).astype(F32)
    earlier = lax.broadcasted_iota(jnp.int32, (256, 256), 0) < lax.broadcasted_iota(
        jnp.int32, (256, 256), 1
    )
    before = jnp.dot(
        onehot.astype(BF16), jnp.where(earlier, 1.0, 0.0).astype(BF16), preferred_element_type=F32
    )
    slot_row = jnp.sum(onehot * before, axis=0, keepdims=True)
    slots = lax.broadcasted_iota(jnp.int32, (128, 256), 0).astype(F32)

    def mask_of(k):
        return jnp.logical_and(id_row == k, slot_row == slots)

    for k in range(4):
        pick[k] = jnp.where(mask_of(k), 1.0, 0.0).astype(BF16)
    for copy in load_tok:
        copy.wait()
    load_cw.wait()
    small = jnp.zeros((4, 256), F32)
    for k in range(8):
        small += lax.dot_general(
            cw[:, 640 * k : 640 * k + 640],
            tok[k],
            (((1,), (1,)), ((), ())),
            preferred_element_type=F32,
        )
    rows[0:4] = small
    for copy in load_out:
        copy.wait()

    def head_add(shard, q):
        cols = slice(128 * q, 128 * q + 128)
        head_o[:, cols] += jnp.dot(tok[shard], wbuf[shard, q], preferred_element_type=F32)

    for q in range(4):
        head_o[:, 128 * q : 128 * q + 128] = jnp.dot(
            tok[b], wbuf[b, q], preferred_element_type=F32
        )

    from_left = [(left, 0), (left, 1), (left, 2), (left, 3), (far, 0), (far, 1)]
    from_right = [(right, 2), (right, 3), (right, 0), (right, 1), (far, 2), (far, 3)]
    flip = 1 - 2 * c

    def w_step(s):
        for side, (shard, q) in enumerate((from_left[s], from_right[s])):
            arrived(wbuf.at[shard, q], wrs.at[shard, q])
            if s < 2:
                start(w_send(shard, q, (right, left)[side], 12 + 2 * s + side))
            start(w_send(shard, q, mate, 16 + 2 * s + side))
        for shard, q in (from_left[s], from_right[s]):
            head_add(shard, q)

    def w_mate(s):
        for shard, q in (from_left[s], from_right[s]):
            arrived(wbuf.at[shard + flip, q], wrs.at[shard + flip, q])
            head_add(shard + flip, q)

    for q in range(4):
        arrived(wbuf.at[mate, q], wrs.at[mate, q])
        head_add(mate, q)
    w_step(0)
    w_step(1)
    w_mate(0)

    z_sends = [
        remote(
            pbuf.at[mine_j],
            pbuf.at[mine_j],
            pzss.at[k - 1],
            pzrs.at[mine_j],
            y * NZ + lax.rem(z + k, NZ),
            b,
        )
        for k in range(1, NZ)
    ]

    def group_send(k):
        g = lax.rem(y + k, NY)
        part = town.at[pl.ds(8 * g, 8), c]
        return remote(part, part, tpss.at[g], tprs.at[g], v, mate)

    @pl.when(owner)
    def _():
        town[v, c] = tv[mine_j, c]
        for k in range(NY):
            g = lax.rem(y + k, NY)

            @pl.loop(0, NZ)
            def _(s):
                @pl.when(8 * g + s != v)
                def _():
                    arrived(town.at[8 * g + s, c], trs.at[8 * g + s])

            group_send(k).start()
        total = jnp.zeros((256, 128), F32)
        for k in range(NY):
            g = lax.rem(y + k, NY)
            part = town.at[pl.ds(8 * g, 8), 1 - c]
            arrived(part, tprs.at[g])
            for h in range(2):
                total += jnp.dot(
                    tok[2 * g + h],
                    town[pl.ds(8 * g + 4 * h, 4)].reshape(640, 128),
                    preferred_element_type=F32,
                )
        rounded = total.astype(BF16)
        low = (
            jnp.where(mine_j >= 10, 1, 0)
            + jnp.where(mine_j >= 15, 1, 0)
            + jnp.where(mine_j >= 18, 1, 0)
        )
        high = (
            jnp.where(mine_j >= 10, 1, 0)
            + jnp.where(mine_j >= 15, 1, 0)
            + jnp.where(mine_j >= 17, 1, 0)
        )
        lane = lax.broadcasted_iota(jnp.int32, (128, 128), 1)
        pbuf[mine_j] = jnp.where(
            lane < 64,
            jnp.dot(pick[low], rounded, preferred_element_type=F32),
            jnp.dot(pick[high], rounded, preferred_element_type=F32),
        ).astype(BF16)
        for copy in z_sends:
            copy.start()

    w_step(2)
    w_mate(1)

    def y_send(j, i, side):
        return remote(
            pbuf.at[j],
            pbuf.at[j],
            pyss.at[i, side],
            pyrs.at[j],
            (y_up, y_down)[side] * NZ + z,
            b,
        )

    def o_send(j, i, side):
        part = pbuf.at[j, pl.ds(64 * side, 64)]
        return remote(part, part, poss.at[i, side], pors.at[j, side], (y_up, y_down)[side] * NZ + z, b)

    for k in range(5):
        i = lax.rem(mine_i + k, 5)
        j = 5 * y + i

        @pl.when(j < TILES)
        def _():
            if k == 0:

                @pl.when(jnp.logical_not(owner))
                def _():
                    arrived(pbuf.at[j], pzrs.at[j])
            else:
                arrived(pbuf.at[j], pzrs.at[j])
            for side in range(2):
                y_send(j, i, side).start()

    w_step(3)
    w_mate(2)
    for i in range(5):
        for side, ring in enumerate((y_down, y_up)):
            j = 5 * ring + i

            @pl.when(j < TILES)
            def _():
                arrived(pbuf.at[j], pyrs.at[j])
                o_send(j, i, side).start()

    w_step(4)
    w_mate(3)
    for i in range(5):
        j = 5 * y_far + i

        @pl.when(j < TILES)
        def _():
            for side in range(2):
                part = pbuf.at[j, pl.ds(64 * side, 64)]
                arrived(part, pors.at[j, side])

    s1_o[...] = jnp.dot(
        jnp.concatenate([pbuf[t] for t in range(10)], axis=1), o1[...], preferred_element_type=F32
    )
    s2_o[...] = jnp.dot(
        jnp.concatenate([pbuf[t] for t in range(10, 15)], axis=1),
        o2[...],
        preferred_element_type=F32,
    )
    split = pbuf[17]
    s3_o[...] = jnp.dot(
        jnp.concatenate([pbuf[15], pbuf[16], split[:, :64]], axis=1),
        o3[...],
        preferred_element_type=F32,
    )
    s4_o[...] = jnp.dot(
        jnp.concatenate([split[:, 64:], pbuf[18][:, :96]], axis=1),
        o4[...],
        preferred_element_type=F32,
    )
    eye = lax.broadcasted_iota(jnp.int32, (128, 128), 0) == lax.broadcasted_iota(
        jnp.int32, (128, 128), 1
    )

    def as_row(col):
        return jnp.sum(jnp.where(eye, col, 0.0), axis=0, keepdims=True)

    def as_col(row):
        return jnp.sum(jnp.where(eye, row, 0.0), axis=1, keepdims=True)

    tail_rows = [as_row(log_sum(ref[...])) for ref in (s1_o, s2_o, s3_o, s4_o)]
    w_step(5)
    w_mate(4)
    w_mate(5)
    head_rows = [as_row(log_sum(head_o[128 * k : 128 * k + 128])) for k in range(2)]
    packed = jnp.concatenate(head_rows + tail_rows + [jnp.zeros((2, 128), F32)], axis=0)
    msg[...] = packed
    xbuf[v] = packed

    def x_send(k):
        to = lax.rem(v + k, NV)
        return remote(msg, xbuf.at[v], xss.at[k], xrs.at[v], to, b)

    @pl.loop(1, NV)
    def _(k):
        x_send(k).start()

    small = rows[0:4]
    small_top = jnp.max(small, axis=0, keepdims=True)
    small_sum = jnp.sum(jnp.exp(small - small_top), axis=0, keepdims=True)

    @pl.loop(1, NV)
    def _(k):
        s = lax.rem(v + k, NV)
        arrived(xbuf.at[s], xrs.at[s])

    every = xbuf[...]
    top = jnp.max(every, axis=0)
    lse = top + jnp.log(jnp.sum(jnp.exp(every - top[None]), axis=0))
    head_lse = jnp.concatenate([lse[0:1], lse[1:2]], axis=1)
    overall = jnp.maximum(head_lse, small_top)
    total_row = overall + jnp.log(
        jnp.exp(head_lse - overall) + small_sum * jnp.exp(small_top - overall)
    )
    lane = lax.broadcasted_iota(jnp.int32, (128, 128), 1)
    found = jnp.zeros((128, 128), F32)
    for k in range(2):
        found = jnp.where(lane == k, as_col(total_row[:, 128 * k : 128 * k + 128]), found)
    for k in range(4):
        mask = mask_of(k)
        slot_logp = jnp.sum(
            jnp.where(mask, small[k : k + 1] - total_row, 0.0), axis=1, keepdims=True
        )
        used = jnp.max(jnp.where(mask, 1.0, 0.0), axis=1, keepdims=True)
        found = jnp.where(lane == 2 + k, as_col(lse[2 + k : 3 + k]) - slot_logp, found)
        found = jnp.where(lane == 6 + k, used, found)
    off_o[...] = found

    for copy in pending:
        copy.wait_send()

    @pl.loop(0, TILES)
    def _(j):
        v_to, copy = t_send(j)

        @pl.when(v_to != v)
        def _():
            copy.wait_send()

    @pl.when(owner)
    def _():
        for k in range(NY):
            group_send(k).wait_send()
        for copy in z_sends:
            copy.wait_send()

    for i in range(5):
        for side in range(2):

            @pl.when(5 * y + i < TILES)
            def _():
                y_send(5 * y + i, i, side).wait_send()

            j = 5 * (y_down, y_up)[side] + i

            @pl.when(j < TILES)
            def _():
                o_send(j, i, side).wait_send()

    @pl.loop(1, NV)
    def _(k):
        x_send(k).wait_send()


def finish(head_i, s1_i, s2_i, s3_i, s4_i, off_i, head_o, s1_o, s2_o, s3_o, s4_o):
    for k in range(2):
        part = slice(128 * k, 128 * k + 128)
        head_o[part] = head_i[part] - off_i[:, k : k + 1]
    for k, (src, dst) in enumerate(((s1_i, s1_o), (s2_i, s2_o), (s3_i, s3_o), (s4_i, s4_o))):
        used = off_i[:, 6 + k : 7 + k] > 0.5
        dst[...] = jnp.where(used, src[...] - off_i[:, 2 + k : 3 + k], 0.0)


def shards(tokens, cluster_ids, head_weight, cluster_weight, tail_proj, o1, o2, o3, o4):
    widths = [(256, 512), (128, 512), (128, 1024), (128, 1024), (128, 1024)]
    shapes = [jax.ShapeDtypeStruct(s, F32) for s in widths]
    dma = pltpu.SemaphoreType.DMA
    hbm = pl.BlockSpec(memory_space=pltpu.HBM)
    vmem = pl.BlockSpec(memory_space=pltpu.VMEM)
    raw = pl.pallas_call(
        work,
        out_shape=shapes + [jax.ShapeDtypeStruct((128, 128), F32)],
        in_specs=[hbm] * 9,
        out_specs=[vmem] * 6,
        scratch_shapes=[
            pltpu.VMEM((8, 256, 640), BF16),
            pltpu.VMEM((1, 256), jnp.int32),
            pltpu.VMEM((NB, 4, 640, 128), BF16),
            pltpu.VMEM((4, 5120), BF16),
            pltpu.VMEM((160, 2400), BF16),
            pltpu.VMEM((TILES, 2, 80, 128), BF16),
            pltpu.VMEM((NV, 2, 80, 128), BF16),
            pltpu.VMEM((TILES, 128, 128), BF16),
            pltpu.VMEM((1280, 512), BF16),
            pltpu.VMEM((640, 1024), BF16),
            pltpu.VMEM((320, 1024), BF16),
            pltpu.VMEM((160, 1024), BF16),
            pltpu.VMEM((8, 128), F32),
            pltpu.VMEM((NV, 8, 128), F32),
            pltpu.VMEM((4, 128, 256), BF16),
            pltpu.VMEM((8, 256), F32),
            dma((4,)),
            dma((8,)),
            dma((7,)),
            dma((28,)),
            dma((NB, 4)),
            dma((TILES,)),
            dma((NV,)),
            dma((NY,)),
            dma((NY,)),
            dma((NZ,)),
            dma((TILES,)),
            dma((5, 2)),
            dma((TILES,)),
            dma((5, 2)),
            dma((TILES, 2)),
            dma((NV,)),
            dma((NV,)),
        ],
        compiler_params=pltpu.CompilerParams(
            collective_id=0, has_side_effects=True, vmem_limit_bytes=48 * 1024 * 1024
        ),
        name="work",
    )(
        tokens,
        cluster_ids.reshape(1, 256),
        head_weight,
        cluster_weight.T,
        tail_proj,
        o1,
        o2,
        o3,
        o4,
    )
    return tuple(
        pl.pallas_call(
            finish,
            out_shape=shapes,
            in_specs=[vmem] * 6,
            out_specs=[vmem] * 5,
            compiler_params=pltpu.CompilerParams(vmem_limit_bytes=16 * 1024 * 1024),
            name="finish",
        )(*raw)
    )


def solution(mesh):
    in_specs = (
        P("batch", None),
        P("batch", None),
        P("batch", "vocab"),
        P(),
        P("vocab", None),
        P(None, "vocab"),
        P(None, "vocab"),
        P(None, "vocab"),
        P(None, "vocab"),
    )
    return jax.shard_map(
        shards, mesh=mesh, in_specs=in_specs, out_specs=(P("batch", "vocab"),) * 5, check_vma=False
    )
```

```python
import jax
import jax.numpy as jnp
from jax import lax
from jax.experimental import pallas as pl
from jax.experimental.pallas import tpu as pltpu
from jax.sharding import PartitionSpec as P

NY, NZ, NX = 4, 8, 4
NV = NY * NZ
NB = 2 * NX
TILES = 19
F32, BF16 = jnp.float32, jnp.bfloat16


def ring_place(i, y):
    return lax.rem((i * 8) // 5 + 2 * y, NZ)


def remote(src, dst, send_sem, recv_sem, v, b):
    return pltpu.make_async_remote_copy(
        src_ref=src,
        dst_ref=dst,
        send_sem=send_sem,
        recv_sem=recv_sem,
        device_id=(v, b),
        device_id_type=pl.DeviceIdType.MESH,
    )


def arrived(ref, sem):
    pltpu.make_async_copy(ref, ref, sem).wait()


def log_sum(x):
    top = jnp.max(x, axis=1, keepdims=True)
    return top + jnp.log(jnp.sum(jnp.exp(x - top), axis=1, keepdims=True))


def work(
    tok_h, ids_h, w_h, cw_h, t_h, o1_h, o2_h, o3_h, o4_h,
    head_o, s1_o, s2_o, s3_o, s4_o, off_o,
    tok, ids, wbuf, cw, tin, tv, town, pbuf, o1, o2, o3, o4, msg, xbuf, pick, rows,
    ld_w, ld_tok, ld_misc,
    wss, wrs, tss, trs, tpss, tprs, pzss, pzrs, pyss, pyrs, poss, pors, xss, xrs,
):
    v, b = lax.axis_index("vocab"), lax.axis_index("batch")
    y, z = v // NZ, lax.rem(v, NZ)
    x, c = b // 2, lax.rem(b, 2)
    right = lax.rem(x + 1, NX) * 2 + c
    left = lax.rem(x + 3, NX) * 2 + c
    far = lax.rem(x + 2, NX) * 2 + c
    mate = x * 2 + 1 - c
    y_up, y_down, y_far = lax.rem(y + 1, NY), lax.rem(y + 3, NY), lax.rem(y + 2, NY)

    load_t = pltpu.make_async_copy(t_h, tin, ld_misc.at[0])
    load_t.start()
    barrier = pltpu.get_barrier_semaphore()
    for peer in (right, left, mate):
        pl.semaphore_signal(barrier, inc=1, device_id=(v, peer), device_id_type=pl.DeviceIdType.MESH)

    @pl.loop(1, NV)
    def _(k):
        pl.semaphore_signal(
            barrier, inc=1, device_id=(lax.rem(v + k, NV), b), device_id_type=pl.DeviceIdType.MESH
        )

    load_w = [
        pltpu.make_async_copy(w_h.at[:, pl.ds(128 * q, 128)], wbuf.at[b, q], ld_w.at[q])
        for q in range(4)
    ]
    for copy in load_w:
        copy.start()
    load_ids = pltpu.make_async_copy(ids_h, ids, ld_misc.at[1])
    load_ids.start()
    load_cw = pltpu.make_async_copy(cw_h, cw, ld_misc.at[2])
    load_cw.start()
    load_tok = [
        pltpu.make_async_copy(tok_h.at[:, pl.ds(640 * k, 640)], tok.at[k], ld_tok.at[k])
        for k in range(8)
    ]
    for copy in load_tok:
        copy.start()
    load_out = [
        pltpu.make_async_copy(src, dst, ld_misc.at[3 + k])
        for k, (src, dst) in enumerate(((o1_h, o1), (o2_h, o2), (o3_h, o3), (o4_h, o4)))
    ]
    for copy in load_out:
        copy.start()

    load_t.wait()
    for j in range(TILES - 1):
        for h in range(2):
            tv[j, h] = tin[80 * h : 80 * h + 80, 128 * j : 128 * j + 128]
    for h in range(2):
        tv[TILES - 1, h] = jnp.concatenate(
            [tin[80 * h : 80 * h + 80, 2304:2400], jnp.zeros((80, 32), BF16)], axis=1
        )
    pl.semaphore_wait(barrier, 3 + NV - 1)

    def t_send(j):
        y_to = j // 5
        v_to = y_to * NZ + ring_place(lax.rem(j, 5), y_to)
        sends = jnp.logical_and(v_to != v, lax.rem(j, 2) == c)
        return sends, remote(tv.at[j], town.at[v], tss.at[j], trs.at[v], v_to, b)

    @pl.loop(0, TILES)
    def _(k):
        sends, copy = t_send(lax.rem(k + v, TILES))

        @pl.when(sends)
        def _():
            copy.start()

    for copy in load_w:
        copy.wait()
    def w_send(shard, q, to, k):
        return remote(wbuf.at[shard, q], wbuf.at[shard, q], wss.at[k], wrs.at[shard, q], v, to)

    pending = []

    def start(copy):
        copy.start()
        pending.append(copy)

    for k in range(4):
        start(w_send(b, k, right, k))
        start(w_send(b, (k + 2) % 4, left, 4 + k))
    for k in range(4):
        start(w_send(b, k, mate, 8 + k))

    mine_r = lax.rem(z - 2 * y + 8, NZ)
    mine_i = (5 * mine_r + 7) // 8
    mine_j = 5 * y + mine_i
    owner = jnp.logical_and((mine_i * 8) // 5 == mine_r, mine_j < TILES)

    load_ids.wait()
    id_row = ids[...]
    kinds = lax.broadcasted_iota(jnp.int32, (8, 256), 0)
    onehot = jnp.where(kinds == id_row, 1.0, 0.0).astype(F32)
    earlier = lax.broadcasted_iota(jnp.int32, (256, 256), 0) < lax.broadcasted_iota(
        jnp.int32, (256, 256), 1
    )
    before = jnp.dot(
        onehot.astype(BF16), jnp.where(earlier, 1.0, 0.0).astype(BF16), preferred_element_type=F32
    )
    slot_row = jnp.sum(onehot * before, axis=0, keepdims=True)
    slots = lax.broadcasted_iota(jnp.int32, (128, 256), 0).astype(F32)

    def mask_of(k):
        return jnp.logical_and(id_row == k, slot_row == slots)

    for k in range(4):
        pick[k] = jnp.where(mask_of(k), 1.0, 0.0).astype(BF16)
    for copy in load_tok:
        copy.wait()
    load_cw.wait()
    small = jnp.zeros((4, 256), F32)
    for k in range(8):
        small += lax.dot_general(
            cw[:, 640 * k : 640 * k + 640],
            tok[k],
            (((1,), (1,)), ((), ())),
            preferred_element_type=F32,
        )
    rows[0:4] = small
    for copy in load_out:
        copy.wait()

    def product(shard, h):
        pair = jnp.concatenate([wbuf[shard, 2 * h], wbuf[shard, 2 * h + 1]], axis=1)
        return jnp.dot(tok[shard], pair, preferred_element_type=F32)

    def head_add(shard, h):
        head_o[:, 256 * h : 256 * h + 256] += product(shard, h)

    for h in range(2):
        head_o[:, 256 * h : 256 * h + 256] = product(b, h)

    from_left = [(left, 0), (left, 1), (left, 2), (left, 3), (far, 0), (far, 1)]
    from_right = [(right, 2), (right, 3), (right, 0), (right, 1), (far, 2), (far, 3)]
    flip = 1 - 2 * c

    def w_take(s):
        for side, (shard, q) in enumerate((from_left[s], from_right[s])):
            arrived(wbuf.at[shard, q], wrs.at[shard, q])
            if s < 2:
                start(w_send(shard, q, (right, left)[side], 12 + 2 * s + side))
            start(w_send(shard, q, mate, 16 + 2 * s + side))

    def w_use(p):
        pairs = (from_left[2 * p : 2 * p + 2], from_right[2 * p : 2 * p + 2])
        for pair in pairs:
            head_add(pair[0][0], pair[0][1] // 2)
        for pair in pairs:
            for shard, q in pair:
                arrived(wbuf.at[shard + flip, q], wrs.at[shard + flip, q])
            head_add(pair[0][0] + flip, pair[0][1] // 2)

    for h in range(2):
        for q in (2 * h, 2 * h + 1):
            arrived(wbuf.at[mate, q], wrs.at[mate, q])
        head_add(mate, h)
    w_take(0)

    z_sends = [
        remote(
            pbuf.at[mine_j],
            pbuf.at[mine_j],
            pzss.at[k - 1],
            pzrs.at[mine_j],
            y * NZ + lax.rem(z + k, NZ),
            b,
        )
        for k in (4, 3, 5, 2, 6, 1, 7)
    ]

    def group_send(k):
        part = town.at[pl.ds(8 * lax.rem(y + k, NY), 8)]
        return remote(part, part, tpss.at[k], tprs.at[k], v, mate)

    first = jnp.logical_and(owner, lax.rem(mine_j, 2) == c)
    second = jnp.logical_and(owner, lax.rem(mine_j, 2) != c)

    @pl.when(first)
    def _():
        town[v] = tv[mine_j]

    @pl.when(owner)
    def _():
        total = jnp.zeros((256, 128), F32)
        for k in range(NY):
            g = lax.rem(y + k, NY)

            @pl.when(first)
            def _():
                @pl.loop(0, NZ)
                def _(s):
                    @pl.when(8 * g + s != v)
                    def _():
                        arrived(town.at[8 * g + s], trs.at[8 * g + s])

                group_send(k).start()

            @pl.when(second)
            def _():
                arrived(town.at[pl.ds(8 * g, 8)], tprs.at[k])

            for h in range(2):
                total += jnp.dot(
                    tok[2 * g + h],
                    town[pl.ds(8 * g + 4 * h, 4)].reshape(640, 128),
                    preferred_element_type=F32,
                )
        rounded = total.astype(BF16)
        low = (
            jnp.where(mine_j >= 10, 1, 0)
            + jnp.where(mine_j >= 15, 1, 0)
            + jnp.where(mine_j >= 18, 1, 0)
        )
        high = (
            jnp.where(mine_j >= 10, 1, 0)
            + jnp.where(mine_j >= 15, 1, 0)
            + jnp.where(mine_j >= 17, 1, 0)
        )
        lane = lax.broadcasted_iota(jnp.int32, (128, 128), 1)
        pbuf[mine_j] = jnp.where(
            lane < 64,
            jnp.dot(pick[low], rounded, preferred_element_type=F32),
            jnp.dot(pick[high], rounded, preferred_element_type=F32),
        ).astype(BF16)
        for copy in z_sends:
            copy.start()

    w_take(1)
    w_take(2)

    def y_send(j, i, side):
        return remote(
            pbuf.at[j],
            pbuf.at[j],
            pyss.at[i, side],
            pyrs.at[j],
            (y_up, y_down)[side] * NZ + z,
            b,
        )

    def o_send(j, i, side):
        part = pbuf.at[j, pl.ds(64 * side, 64)]
        return remote(part, part, poss.at[i, side], pors.at[j, side], (y_up, y_down)[side] * NZ + z, b)

    def relay_z(i):
        j = 5 * y + i

        @pl.when(jnp.logical_and(j < TILES, jnp.logical_not(jnp.logical_and(owner, mine_i == i))))
        def _():
            arrived(pbuf.at[j], pzrs.at[j])

        @pl.when(j < TILES)
        def _():
            for side in range(2):
                y_send(j, i, side).start()

    def relay_y(i):
        for side, ring in enumerate((y_down, y_up)):
            j = 5 * ring + i

            @pl.when(j < TILES)
            def _():
                arrived(pbuf.at[j], pyrs.at[j])
                o_send(j, i, side).start()

    for i in range(5):
        relay_z(i)
        if i == 2:
            w_use(0)
            w_take(3)
    w_use(1)
    for i in range(5):
        relay_y(i)
        if i == 2:
            w_take(4)
    w_take(5)
    eye = lax.broadcasted_iota(jnp.int32, (128, 128), 0) == lax.broadcasted_iota(
        jnp.int32, (128, 128), 1
    )

    def as_row(col):
        return jnp.sum(jnp.where(eye, col, 0.0), axis=0, keepdims=True)

    def as_col(row):
        return jnp.sum(jnp.where(eye, row, 0.0), axis=1, keepdims=True)

    def tiles(lo, hi):
        return jnp.concatenate([pbuf[t] for t in range(lo, hi)], axis=1)

    def score(ring):
        if ring < 2:
            s1_o[...] += jnp.dot(
                tiles(5 * ring, 5 * ring + 5),
                o1[640 * ring : 640 * ring + 640],
                preferred_element_type=F32,
            )
        elif ring == 2:
            s2_o[...] = jnp.dot(tiles(10, 15), o2[...], preferred_element_type=F32)
        else:
            split = pbuf[17]
            s3_o[...] = jnp.dot(
                jnp.concatenate([tiles(15, 17), split[:, :64]], axis=1),
                o3[...],
                preferred_element_type=F32,
            )
            s4_o[...] = jnp.dot(
                jnp.concatenate([split[:, 64:], pbuf[18][:, :96]], axis=1),
                o4[...],
                preferred_element_type=F32,
            )

    s1_o[...] = jnp.zeros_like(s1_o)
    for ring in range(NY):
        pl.when(y_far != ring)(lambda: score(ring))
    w_use(2)
    head_rows = [as_row(log_sum(head_o[128 * k : 128 * k + 128])) for k in range(2)]
    for i in range(5):
        j = 5 * y_far + i

        @pl.when(j < TILES)
        def _():
            for side in range(2):
                part = pbuf.at[j, pl.ds(64 * side, 64)]
                arrived(part, pors.at[j, side])

    for ring in range(NY):
        pl.when(y_far == ring)(lambda: score(ring))
    tail_rows = [as_row(log_sum(ref[...])) for ref in (s1_o, s2_o, s3_o, s4_o)]
    packed = jnp.concatenate(head_rows + tail_rows + [jnp.zeros((2, 128), F32)], axis=0)
    msg[...] = packed
    xbuf[v] = packed

    def x_send(k):
        to = lax.rem(v + k, NV)
        return remote(msg, xbuf.at[v], xss.at[k], xrs.at[v], to, b)

    @pl.loop(1, NV)
    def _(k):
        x_send(k).start()

    small = rows[0:4]
    small_top = jnp.max(small, axis=0, keepdims=True)
    small_sum = jnp.sum(jnp.exp(small - small_top), axis=0, keepdims=True)

    for copy in pending:
        copy.wait_send()

    @pl.loop(0, TILES)
    def _(j):
        sends, copy = t_send(j)

        @pl.when(sends)
        def _():
            copy.wait_send()

    @pl.when(first)
    def _():
        for k in range(NY):
            group_send(k).wait_send()

    @pl.when(owner)
    def _():
        for copy in z_sends:
            copy.wait_send()

    for i in range(5):
        for side in range(2):

            @pl.when(5 * y + i < TILES)
            def _():
                y_send(5 * y + i, i, side).wait_send()

            j = 5 * (y_down, y_up)[side] + i

            @pl.when(j < TILES)
            def _():
                o_send(j, i, side).wait_send()

    @pl.loop(1, NV)
    def _(k):
        s = lax.rem(v + k, NV)
        arrived(xbuf.at[s], xrs.at[s])

    every = xbuf[...]
    top = jnp.max(every, axis=0)
    lse = top + jnp.log(jnp.sum(jnp.exp(every - top[None]), axis=0))
    head_lse = jnp.concatenate([lse[0:1], lse[1:2]], axis=1)
    overall = jnp.maximum(head_lse, small_top)
    total_row = overall + jnp.log(
        jnp.exp(head_lse - overall) + small_sum * jnp.exp(small_top - overall)
    )
    lane = lax.broadcasted_iota(jnp.int32, (128, 128), 1)
    found = jnp.zeros((128, 128), F32)
    for k in range(2):
        found = jnp.where(lane == k, as_col(total_row[:, 128 * k : 128 * k + 128]), found)
    for k in range(4):
        mask = mask_of(k)
        slot_logp = jnp.sum(
            jnp.where(mask, small[k : k + 1] - total_row, 0.0), axis=1, keepdims=True
        )
        used = jnp.max(jnp.where(mask, 1.0, 0.0), axis=1, keepdims=True)
        found = jnp.where(lane == 2 + k, as_col(lse[2 + k : 3 + k]) - slot_logp, found)
        found = jnp.where(lane == 6 + k, used, found)
    off_o[...] = found

    @pl.loop(1, NV)
    def _(k):
        x_send(k).wait_send()


def finish(
    head_i, s1_i, s2_i, s3_i, s4_i, off_i,
    head_o, s1_o, s2_o, s3_o, s4_o,
    head_v, s1_v, s2_v, s3_v, s4_v, sems,
):
    copies = []

    def write(src, dst, sem):
        copies.append(pltpu.make_async_copy(src, dst, sem))
        copies[-1].start()

    for k in range(2):
        part = slice(128 * k, 128 * k + 128)
        head_v[part] = head_i[part] - off_i[:, k : k + 1]
        write(head_v.at[part], head_o.at[part], sems.at[k])
    tails = ((s2_i, s2_v, s2_o), (s3_i, s3_v, s3_o), (s4_i, s4_v, s4_o), (s1_i, s1_v, s1_o))
    for at, (src, held, dst) in zip((1, 2, 3, 0), tails):
        used = off_i[:, 6 + at : 7 + at] > 0.5
        held[...] = jnp.where(used, src[...] - off_i[:, 2 + at : 3 + at], 0.0)
        write(held, dst, sems.at[2 + at])
    for copy in copies:
        copy.wait()


def shards(tokens, cluster_ids, head_weight, cluster_weight, tail_proj, o1, o2, o3, o4):
    widths = [(256, 512), (128, 512), (128, 1024), (128, 1024), (128, 1024)]
    shapes = [jax.ShapeDtypeStruct(s, F32) for s in widths]
    held = [pltpu.VMEM(s, F32) for s in widths + [(128, 128)]]
    dma = pltpu.SemaphoreType.DMA
    hbm = pl.BlockSpec(memory_space=pltpu.HBM)
    vmem = pl.BlockSpec(memory_space=pltpu.VMEM)
    raw = pl.pallas_call(
        work,
        out_shape=held,
        in_specs=[hbm] * 9,
        out_specs=[vmem] * 6,
        scratch_shapes=[
            pltpu.VMEM((8, 256, 640), BF16),
            pltpu.VMEM((1, 256), jnp.int32),
            pltpu.VMEM((NB, 4, 640, 128), BF16),
            pltpu.VMEM((4, 5120), BF16),
            pltpu.VMEM((160, 2400), BF16),
            pltpu.VMEM((TILES, 2, 80, 128), BF16),
            pltpu.VMEM((NV, 2, 80, 128), BF16),
            pltpu.VMEM((TILES, 128, 128), BF16),
            pltpu.VMEM((1280, 512), BF16),
            pltpu.VMEM((640, 1024), BF16),
            pltpu.VMEM((320, 1024), BF16),
            pltpu.VMEM((160, 1024), BF16),
            pltpu.VMEM((8, 128), F32),
            pltpu.VMEM((NV, 8, 128), F32),
            pltpu.VMEM((4, 128, 256), BF16),
            pltpu.VMEM((8, 256), F32),
            dma((4,)),
            dma((8,)),
            dma((7,)),
            dma((28,)),
            dma((NB, 4)),
            dma((TILES,)),
            dma((NV,)),
            dma((NY,)),
            dma((NY,)),
            dma((NZ,)),
            dma((TILES,)),
            dma((5, 2)),
            dma((TILES,)),
            dma((5, 2)),
            dma((TILES, 2)),
            dma((NV,)),
            dma((NV,)),
        ],
        compiler_params=pltpu.CompilerParams(
            collective_id=0, has_side_effects=True, vmem_limit_bytes=67043328 - 2560 * 1024
        ),
        name="work",
    )(
        tokens,
        cluster_ids.reshape(1, 256),
        head_weight,
        cluster_weight.T,
        tail_proj,
        o1,
        o2,
        o3,
        o4,
    )
    return tuple(
        pl.pallas_call(
            finish,
            out_shape=shapes,
            in_specs=[vmem] * 6,
            out_specs=[hbm] * 5,
            scratch_shapes=[pltpu.VMEM(s, F32) for s in widths] + [dma((6,))],
            compiler_params=pltpu.CompilerParams(vmem_limit_bytes=16 * 1024 * 1024),
            name="finish",
        )(*raw)
    )


def solution(mesh):
    in_specs = (
        P("batch", None),
        P("batch", None),
        P("batch", "vocab"),
        P(),
        P("vocab", None),
        P(None, "vocab"),
        P(None, "vocab"),
        P(None, "vocab"),
        P(None, "vocab"),
    )
    return jax.shard_map(
        shards, mesh=mesh, in_specs=in_specs, out_specs=(P("batch", "vocab"),) * 5, check_vma=False
    )
```

```python
import jax
import jax.numpy as jnp
from jax import lax
from jax.experimental import pallas as pl
from jax.experimental.pallas import tpu as pltpu
from jax.sharding import PartitionSpec as P

NY, NZ, NX = 4, 8, 4
NV = NY * NZ
NB = 2 * NX
TILES = 19
F32, BF16 = jnp.float32, jnp.bfloat16


def ring_place(i, y):
    return lax.rem((i * 8) // 5 + 2 * y, NZ)


def remote(src, dst, send_sem, recv_sem, v, b):
    return pltpu.make_async_remote_copy(
        src_ref=src,
        dst_ref=dst,
        send_sem=send_sem,
        recv_sem=recv_sem,
        device_id=(v, b),
        device_id_type=pl.DeviceIdType.MESH,
    )


def arrived(ref, sem):
    pltpu.make_async_copy(ref, ref, sem).wait()


def log_sum(x):
    top = jnp.max(x, axis=1, keepdims=True)
    return top + jnp.log(jnp.sum(jnp.exp(x - top), axis=1, keepdims=True))


def work(
    tok_h, ids_h, w_h, cw_h, t_h, o1_h, o2_h, o3_h, o4_h,
    head_o, s1_o, s2_o, s3_o, s4_o, off_o,
    tok, ids, wbuf, cw, tin, tv, town, pbuf, o1, o2, o3, o4, msg, xbuf, pick, wide, known, rows,
    ld_w, ld_tok, ld_misc,
    wss, wrs, tss, trs, tpss, tprs, pzss, pzrs, pyss, pyrs, poss, pors, xss, xrs,
):
    v, b = lax.axis_index("vocab"), lax.axis_index("batch")
    y, z = v // NZ, lax.rem(v, NZ)
    x, c = b // 2, lax.rem(b, 2)
    right = lax.rem(x + 1, NX) * 2 + c
    left = lax.rem(x + 3, NX) * 2 + c
    far = lax.rem(x + 2, NX) * 2 + c
    mate = x * 2 + 1 - c
    y_up, y_down, y_far = lax.rem(y + 1, NY), lax.rem(y + 3, NY), lax.rem(y + 2, NY)

    load_t = pltpu.make_async_copy(t_h, tin, ld_misc.at[0])
    load_t.start()
    barrier = pltpu.get_barrier_semaphore()
    for peer in (right, left, mate):
        pl.semaphore_signal(barrier, inc=1, device_id=(v, peer), device_id_type=pl.DeviceIdType.MESH)

    @pl.loop(1, NV)
    def _(k):
        pl.semaphore_signal(
            barrier, inc=1, device_id=(lax.rem(v + k, NV), b), device_id_type=pl.DeviceIdType.MESH
        )

    load_w = [
        pltpu.make_async_copy(w_h.at[:, pl.ds(128 * q, 128)], wbuf.at[b, q], ld_w.at[q])
        for q in range(4)
    ]
    for copy in load_w:
        copy.start()
    load_ids = pltpu.make_async_copy(ids_h, ids, ld_misc.at[1])
    load_ids.start()
    load_cw = pltpu.make_async_copy(cw_h, cw, ld_misc.at[2])
    load_cw.start()
    load_tok = [
        pltpu.make_async_copy(tok_h.at[:, pl.ds(640 * k, 640)], tok.at[k], ld_tok.at[k])
        for k in range(8)
    ]
    for copy in load_tok:
        copy.start()
    load_out = [
        pltpu.make_async_copy(src, dst, ld_misc.at[3 + k])
        for k, (src, dst) in enumerate(((o1_h, o1), (o2_h, o2), (o3_h, o3), (o4_h, o4)))
    ]
    for copy in load_out:
        copy.start()

    load_t.wait()
    for j in range(TILES - 1):
        for h in range(2):
            tv[j, h] = tin[80 * h : 80 * h + 80, 128 * j : 128 * j + 128]
    for h in range(2):
        tv[TILES - 1, h] = jnp.concatenate(
            [tin[80 * h : 80 * h + 80, 2304:2400], jnp.zeros((80, 32), BF16)], axis=1
        )
    pl.semaphore_wait(barrier, 3 + NV - 1)

    def t_send(j):
        y_to = j // 5
        v_to = y_to * NZ + ring_place(lax.rem(j, 5), y_to)
        sends = jnp.logical_and(v_to != v, lax.rem(j, 2) == c)
        return sends, remote(tv.at[j], town.at[v], tss.at[j], trs.at[v], v_to, b)

    @pl.loop(0, TILES)
    def _(k):
        sends, copy = t_send(lax.rem(k + v, TILES))

        @pl.when(sends)
        def _():
            copy.start()

    for copy in load_w:
        copy.wait()
    def w_send(shard, q, to, k):
        return remote(wbuf.at[shard, q], wbuf.at[shard, q], wss.at[k], wrs.at[shard, q], v, to)

    pending = []

    def start(copy):
        copy.start()
        pending.append(copy)

    for k in range(4):
        start(w_send(b, k, right, k))
        start(w_send(b, (k + 2) % 4, left, 4 + k))
    for k in range(4):
        start(w_send(b, k, mate, 8 + k))

    mine_r = lax.rem(z - 2 * y + 8, NZ)
    mine_i = (5 * mine_r + 7) // 8
    mine_j = 5 * y + mine_i
    owner = jnp.logical_and((mine_i * 8) // 5 == mine_r, mine_j < TILES)

    load_ids.wait()
    id_row = ids[...]
    kinds = lax.broadcasted_iota(jnp.int32, (8, 256), 0)
    onehot = jnp.where(kinds == id_row, 1.0, 0.0).astype(F32)
    earlier = lax.broadcasted_iota(jnp.int32, (256, 256), 0) < lax.broadcasted_iota(
        jnp.int32, (256, 256), 1
    )
    before = jnp.dot(
        onehot.astype(BF16), jnp.where(earlier, 1.0, 0.0).astype(BF16), preferred_element_type=F32
    )
    slot_row = jnp.sum(onehot * before, axis=0, keepdims=True)
    slots = lax.broadcasted_iota(jnp.int32, (128, 256), 0).astype(F32)

    def mask_of(k):
        return jnp.logical_and(id_row == k, slot_row == slots)

    for k in range(4):
        chosen = jnp.where(mask_of(k), 1.0, 0.0)
        wide[k] = chosen
        pick[k] = chosen.astype(BF16)
    for copy in load_tok:
        copy.wait()
    load_cw.wait()
    small = jnp.zeros((4, 256), F32)
    for k in range(8):
        small += lax.dot_general(
            cw[:, 640 * k : 640 * k + 640],
            tok[k],
            (((1,), (1,)), ((), ())),
            preferred_element_type=F32,
        )
    small_top = jnp.max(small, axis=0, keepdims=True)
    rows[0:1] = small_top
    rows[1:2] = jnp.sum(jnp.exp(small - small_top), axis=0, keepdims=True)
    lane = lax.broadcasted_iota(jnp.int32, (128, 128), 1)
    before_lse = jnp.zeros((128, 128), F32)
    for k in range(4):
        logit = jnp.sum(wide[k] * small[k : k + 1], axis=1, keepdims=True)
        used = jnp.sum(wide[k], axis=1, keepdims=True)
        before_lse = jnp.where(lane == 2 + k, -logit, before_lse)
        before_lse = jnp.where(lane == 6 + k, used, before_lse)
    known[...] = before_lse
    for copy in load_out:
        copy.wait()

    def product(shard, h):
        pair = jnp.concatenate([wbuf[shard, 2 * h], wbuf[shard, 2 * h + 1]], axis=1)
        return jnp.dot(tok[shard], pair, preferred_element_type=F32)

    def head_add(shard, h):
        head_o[:, 256 * h : 256 * h + 256] += product(shard, h)

    for h in range(2):
        head_o[:, 256 * h : 256 * h + 256] = product(b, h)

    from_left = [(left, 0), (left, 1), (left, 2), (left, 3), (far, 0), (far, 1)]
    from_right = [(right, 2), (right, 3), (right, 0), (right, 1), (far, 2), (far, 3)]
    flip = 1 - 2 * c

    def w_take(s):
        for side, (shard, q) in enumerate((from_left[s], from_right[s])):
            arrived(wbuf.at[shard, q], wrs.at[shard, q])
            if s < 2:
                start(w_send(shard, q, (right, left)[side], 12 + 2 * s + side))
            start(w_send(shard, q, mate, 16 + 2 * s + side))

    def w_use(p):
        pairs = (from_left[2 * p : 2 * p + 2], from_right[2 * p : 2 * p + 2])
        for pair in pairs:
            head_add(pair[0][0], pair[0][1] // 2)
        for pair in pairs:
            for shard, q in pair:
                arrived(wbuf.at[shard + flip, q], wrs.at[shard + flip, q])
            head_add(pair[0][0] + flip, pair[0][1] // 2)

    for h in range(2):
        for q in (2 * h, 2 * h + 1):
            arrived(wbuf.at[mate, q], wrs.at[mate, q])
        head_add(mate, h)
    w_take(0)

    z_sends = [
        remote(
            pbuf.at[mine_j],
            pbuf.at[mine_j],
            pzss.at[k - 1],
            pzrs.at[mine_j],
            y * NZ + lax.rem(z + k, NZ),
            b,
        )
        for k in (4, 3, 5, 2, 6, 1, 7)
    ]

    def group_send(k):
        part = town.at[pl.ds(8 * lax.rem(y + k, NY), 8)]
        return remote(part, part, tpss.at[k], tprs.at[k], v, mate)

    first = jnp.logical_and(owner, lax.rem(mine_j, 2) == c)
    second = jnp.logical_and(owner, lax.rem(mine_j, 2) != c)

    @pl.when(first)
    def _():
        town[v] = tv[mine_j]

    @pl.when(owner)
    def _():
        total = jnp.zeros((256, 128), F32)
        for k in range(NY):
            g = lax.rem(y + k, NY)

            @pl.when(first)
            def _():
                @pl.loop(0, NZ)
                def _(s):
                    @pl.when(8 * g + s != v)
                    def _():
                        arrived(town.at[8 * g + s], trs.at[8 * g + s])

                group_send(k).start()

            @pl.when(second)
            def _():
                arrived(town.at[pl.ds(8 * g, 8)], tprs.at[k])

            for h in range(2):
                total += jnp.dot(
                    tok[2 * g + h],
                    town[pl.ds(8 * g + 4 * h, 4)].reshape(640, 128),
                    preferred_element_type=F32,
                )
        rounded = total.astype(BF16)
        low = (
            jnp.where(mine_j >= 10, 1, 0)
            + jnp.where(mine_j >= 15, 1, 0)
            + jnp.where(mine_j >= 18, 1, 0)
        )
        high = (
            jnp.where(mine_j >= 10, 1, 0)
            + jnp.where(mine_j >= 15, 1, 0)
            + jnp.where(mine_j >= 17, 1, 0)
        )
        lane = lax.broadcasted_iota(jnp.int32, (128, 128), 1)
        pbuf[mine_j] = jnp.where(
            lane < 64,
            jnp.dot(pick[low], rounded, preferred_element_type=F32),
            jnp.dot(pick[high], rounded, preferred_element_type=F32),
        ).astype(BF16)
        for copy in z_sends:
            copy.start()

    w_take(1)
    w_take(2)

    def y_send(j, i, side):
        return remote(
            pbuf.at[j],
            pbuf.at[j],
            pyss.at[i, side],
            pyrs.at[j],
            (y_up, y_down)[side] * NZ + z,
            b,
        )

    def o_send(j, i, side):
        part = pbuf.at[j, pl.ds(64 * side, 64)]
        return remote(part, part, poss.at[i, side], pors.at[j, side], (y_up, y_down)[side] * NZ + z, b)

    def relay_z(i):
        j = 5 * y + i

        @pl.when(jnp.logical_and(j < TILES, jnp.logical_not(jnp.logical_and(owner, mine_i == i))))
        def _():
            arrived(pbuf.at[j], pzrs.at[j])

        @pl.when(j < TILES)
        def _():
            for side in range(2):
                y_send(j, i, side).start()

    def relay_y(i):
        for side, ring in enumerate((y_down, y_up)):
            j = 5 * ring + i

            @pl.when(j < TILES)
            def _():
                arrived(pbuf.at[j], pyrs.at[j])
                o_send(j, i, side).start()

    for i in range(5):
        relay_z(i)
        if i == 2:
            w_use(0)
            w_take(3)
    w_use(1)
    for i in range(5):
        relay_y(i)
        if i == 2:
            w_take(4)
    w_take(5)
    eye = lax.broadcasted_iota(jnp.int32, (128, 128), 0) == lax.broadcasted_iota(
        jnp.int32, (128, 128), 1
    )

    def as_row(col):
        return jnp.sum(jnp.where(eye, col, 0.0), axis=0, keepdims=True)

    def as_col(row):
        return jnp.sum(jnp.where(eye, row, 0.0), axis=1, keepdims=True)

    def tiles(lo, hi):
        return jnp.concatenate([pbuf[t] for t in range(lo, hi)], axis=1)

    def score(ring):
        if ring < 2:
            s1_o[...] += jnp.dot(
                tiles(5 * ring, 5 * ring + 5),
                o1[640 * ring : 640 * ring + 640],
                preferred_element_type=F32,
            )
        elif ring == 2:
            s2_o[...] = jnp.dot(tiles(10, 15), o2[...], preferred_element_type=F32)
        else:
            split = pbuf[17]
            s3_o[...] = jnp.dot(
                jnp.concatenate([tiles(15, 17), split[:, :64]], axis=1),
                o3[...],
                preferred_element_type=F32,
            )
            s4_o[...] = jnp.dot(
                jnp.concatenate([split[:, 64:], pbuf[18][:, :96]], axis=1),
                o4[...],
                preferred_element_type=F32,
            )

    s1_o[...] = jnp.zeros_like(s1_o)
    for ring in range(NY):
        pl.when(y_far != ring)(lambda: score(ring))
    w_use(2)
    head_rows = [as_row(log_sum(head_o[128 * k : 128 * k + 128])) for k in range(2)]
    for i in range(5):
        j = 5 * y_far + i

        @pl.when(j < TILES)
        def _():
            for side in range(2):
                part = pbuf.at[j, pl.ds(64 * side, 64)]
                arrived(part, pors.at[j, side])

    for ring in range(NY):
        pl.when(y_far == ring)(lambda: score(ring))
    tail_rows = [as_row(log_sum(ref[...])) for ref in (s1_o, s2_o, s3_o, s4_o)]
    packed = jnp.concatenate(head_rows + tail_rows + [jnp.zeros((2, 128), F32)], axis=0)
    msg[...] = packed
    xbuf[v] = packed

    def x_send(k):
        to = lax.rem(v + k, NV)
        return remote(msg, xbuf.at[v], xss.at[k], xrs.at[v], to, b)

    @pl.loop(1, NV)
    def _(k):
        x_send(k).start()

    for copy in pending:
        copy.wait_send()

    @pl.loop(0, TILES)
    def _(j):
        sends, copy = t_send(j)

        @pl.when(sends)
        def _():
            copy.wait_send()

    @pl.when(first)
    def _():
        for k in range(NY):
            group_send(k).wait_send()

    @pl.when(owner)
    def _():
        for copy in z_sends:
            copy.wait_send()

    for i in range(5):
        for side in range(2):

            @pl.when(5 * y + i < TILES)
            def _():
                y_send(5 * y + i, i, side).wait_send()

            j = 5 * (y_down, y_up)[side] + i

            @pl.when(j < TILES)
            def _():
                o_send(j, i, side).wait_send()

    @pl.loop(1, NV)
    def _(k):
        s = lax.rem(v + k, NV)
        arrived(xbuf.at[s], xrs.at[s])

    every = xbuf[...]
    top = jnp.max(every, axis=0)
    lse = top + jnp.log(jnp.sum(jnp.exp(every - top[None]), axis=0))
    head_lse = jnp.concatenate([lse[0:1], lse[1:2]], axis=1)
    small_top, small_sum = rows[0:1], rows[1:2]
    overall = jnp.maximum(head_lse, small_top)
    total_row = overall + jnp.log(
        jnp.exp(head_lse - overall) + small_sum * jnp.exp(small_top - overall)
    )
    found = known[...]
    for k in range(2):
        found = jnp.where(lane == k, as_col(total_row[:, 128 * k : 128 * k + 128]), found)
    for k in range(4):
        both = jnp.where(eye, lse[2 + k : 3 + k], 0.0)
        for h in range(2):
            part = slice(128 * h, 128 * h + 128)
            both += wide[k, :, part] * total_row[:, part]
        found += jnp.where(lane == 2 + k, jnp.sum(both, axis=1, keepdims=True), 0.0)
    off_o[...] = found

    @pl.loop(1, NV)
    def _(k):
        x_send(k).wait_send()


def finish(
    head_i, s1_i, s2_i, s3_i, s4_i, off_i,
    head_o, s1_o, s2_o, s3_o, s4_o,
    head_v, s1_v, s2_v, s3_v, s4_v, sems,
):
    copies = []

    def write(src, dst, sem):
        copies.append(pltpu.make_async_copy(src, dst, sem))
        copies[-1].start()

    for k in range(2):
        part = slice(128 * k, 128 * k + 128)
        head_v[part] = head_i[part] - off_i[:, k : k + 1]
        write(head_v.at[part], head_o.at[part], sems.at[k])
    tails = ((s2_i, s2_v, s2_o), (s3_i, s3_v, s3_o), (s4_i, s4_v, s4_o), (s1_i, s1_v, s1_o))
    for at, (src, held, dst) in zip((1, 2, 3, 0), tails):
        used = off_i[:, 6 + at : 7 + at] > 0.5
        held[...] = jnp.where(used, src[...] - off_i[:, 2 + at : 3 + at], 0.0)
        write(held, dst, sems.at[2 + at])
    for copy in copies:
        copy.wait()


def shards(tokens, cluster_ids, head_weight, cluster_weight, tail_proj, o1, o2, o3, o4):
    widths = [(256, 512), (128, 512), (128, 1024), (128, 1024), (128, 1024)]
    shapes = [jax.ShapeDtypeStruct(s, F32) for s in widths]
    held = [pltpu.VMEM(s, F32) for s in widths + [(128, 128)]]
    dma = pltpu.SemaphoreType.DMA
    hbm = pl.BlockSpec(memory_space=pltpu.HBM)
    vmem = pl.BlockSpec(memory_space=pltpu.VMEM)
    raw = pl.pallas_call(
        work,
        out_shape=held,
        in_specs=[hbm] * 9,
        out_specs=[vmem] * 6,
        scratch_shapes=[
            pltpu.VMEM((8, 256, 640), BF16),
            pltpu.VMEM((1, 256), jnp.int32),
            pltpu.VMEM((NB, 4, 640, 128), BF16),
            pltpu.VMEM((4, 5120), BF16),
            pltpu.VMEM((160, 2400), BF16),
            pltpu.VMEM((TILES, 2, 80, 128), BF16),
            pltpu.VMEM((NV, 2, 80, 128), BF16),
            pltpu.VMEM((TILES, 128, 128), BF16),
            pltpu.VMEM((1280, 512), BF16),
            pltpu.VMEM((640, 1024), BF16),
            pltpu.VMEM((320, 1024), BF16),
            pltpu.VMEM((160, 1024), BF16),
            pltpu.VMEM((8, 128), F32),
            pltpu.VMEM((NV, 8, 128), F32),
            pltpu.VMEM((4, 128, 256), BF16),
            pltpu.VMEM((4, 128, 256), F32),
            pltpu.VMEM((128, 128), F32),
            pltpu.VMEM((8, 256), F32),
            dma((4,)),
            dma((8,)),
            dma((7,)),
            dma((28,)),
            dma((NB, 4)),
            dma((TILES,)),
            dma((NV,)),
            dma((NY,)),
            dma((NY,)),
            dma((NZ,)),
            dma((TILES,)),
            dma((5, 2)),
            dma((TILES,)),
            dma((5, 2)),
            dma((TILES, 2)),
            dma((NV,)),
            dma((NV,)),
        ],
        compiler_params=pltpu.CompilerParams(
            collective_id=0, has_side_effects=True, vmem_limit_bytes=67043328 - 2560 * 1024
        ),
        name="work",
    )(
        tokens,
        cluster_ids.reshape(1, 256),
        head_weight,
        cluster_weight.T,
        tail_proj,
        o1,
        o2,
        o3,
        o4,
    )
    return tuple(
        pl.pallas_call(
            finish,
            out_shape=shapes,
            in_specs=[vmem] * 6,
            out_specs=[hbm] * 5,
            scratch_shapes=[pltpu.VMEM(s, F32) for s in widths] + [dma((6,))],
            compiler_params=pltpu.CompilerParams(vmem_limit_bytes=16 * 1024 * 1024),
            name="finish",
        )(*raw)
    )


def solution(mesh):
    in_specs = (
        P("batch", None),
        P("batch", None),
        P("batch", "vocab"),
        P(),
        P("vocab", None),
        P(None, "vocab"),
        P(None, "vocab"),
        P(None, "vocab"),
        P(None, "vocab"),
    )
    return jax.shard_map(
        shards, mesh=mesh, in_specs=in_specs, out_specs=(P("batch", "vocab"),) * 5, check_vma=False
    )
```

```python
import jax
import jax.numpy as jnp
from jax import lax
from jax.experimental import pallas as pl
from jax.experimental.pallas import tpu as pltpu
from jax.sharding import PartitionSpec as P

NY, NZ, NX = 4, 8, 4
NV = NY * NZ
NB = 2 * NX
TILES = 19
F32, BF16 = jnp.float32, jnp.bfloat16


def ring_place(i, y):
    return lax.rem((i * 8) // 5 + 2 * y, NZ)


def remote(src, dst, send_sem, recv_sem, v, b):
    return pltpu.make_async_remote_copy(
        src_ref=src,
        dst_ref=dst,
        send_sem=send_sem,
        recv_sem=recv_sem,
        device_id=(v, b),
        device_id_type=pl.DeviceIdType.MESH,
    )


def arrived(ref, sem):
    pltpu.make_async_copy(ref, ref, sem).wait()


def log_sum(x):
    top = jnp.max(x, axis=1, keepdims=True)
    return top + jnp.log(jnp.sum(jnp.exp(x - top), axis=1, keepdims=True))


def work(
    tok_h, ids_h, w_h, cw_h, t_h, o1_h, o2_h, o3_h, o4_h,
    head_o, s1_o, s2_o, s3_o, s4_o, off_o,
    tok, ids, wbuf, cw, tin, tv, town, pbuf, o1, o2, o3, o4, msg, xbuf, pick, wide, known, rows,
    ld_w, ld_tok, ld_misc,
    wss, wrs, tss, trs, tpss, tprs, pzss, pzrs, pyss, pyrs, poss, pors, xss, xrs,
):
    v, b = lax.axis_index("vocab"), lax.axis_index("batch")
    y, z = v // NZ, lax.rem(v, NZ)
    x, c = b // 2, lax.rem(b, 2)
    right = lax.rem(x + 1, NX) * 2 + c
    left = lax.rem(x + 3, NX) * 2 + c
    far = lax.rem(x + 2, NX) * 2 + c
    mate = x * 2 + 1 - c
    y_up, y_down, y_far = lax.rem(y + 1, NY), lax.rem(y + 3, NY), lax.rem(y + 2, NY)

    load_t = pltpu.make_async_copy(t_h, tin, ld_misc.at[0])
    load_t.start()
    barrier = pltpu.get_barrier_semaphore()
    for peer in (right, left, mate):
        pl.semaphore_signal(barrier, inc=1, device_id=(v, peer), device_id_type=pl.DeviceIdType.MESH)

    @pl.loop(1, NV)
    def _(k):
        pl.semaphore_signal(
            barrier, inc=1, device_id=(lax.rem(v + k, NV), b), device_id_type=pl.DeviceIdType.MESH
        )

    load_w = [
        pltpu.make_async_copy(w_h.at[:, pl.ds(128 * q, 128)], wbuf.at[b, q], ld_w.at[q])
        for q in range(4)
    ]
    for copy in load_w:
        copy.start()
    load_ids = pltpu.make_async_copy(ids_h, ids, ld_misc.at[1])
    load_ids.start()
    load_cw = pltpu.make_async_copy(cw_h, cw, ld_misc.at[2])
    load_cw.start()
    load_tok = [
        pltpu.make_async_copy(tok_h.at[:, pl.ds(640 * k, 640)], tok.at[k], ld_tok.at[k])
        for k in range(8)
    ]
    for copy in load_tok:
        copy.start()
    load_out = [
        pltpu.make_async_copy(src, dst, ld_misc.at[3 + k])
        for k, (src, dst) in enumerate(((o1_h, o1), (o2_h, o2), (o3_h, o3), (o4_h, o4)))
    ]
    for copy in load_out:
        copy.start()

    load_t.wait()
    for j in range(TILES - 1):
        for h in range(2):
            tv[j, h] = tin[80 * h : 80 * h + 80, 128 * j : 128 * j + 128]
    for h in range(2):
        tv[TILES - 1, h] = jnp.concatenate(
            [tin[80 * h : 80 * h + 80, 2304:2400], jnp.zeros((80, 32), BF16)], axis=1
        )
    pl.semaphore_wait(barrier, 3 + NV - 1)

    def t_send(j):
        y_to = j // 5
        v_to = y_to * NZ + ring_place(lax.rem(j, 5), y_to)
        sends = jnp.logical_and(v_to != v, lax.rem(j, 2) == c)
        return sends, remote(tv.at[j], town.at[v], tss.at[j], trs.at[v], v_to, b)

    @pl.loop(0, TILES)
    def _(k):
        sends, copy = t_send(lax.rem(k + v, TILES))

        @pl.when(sends)
        def _():
            copy.start()

    for copy in load_w:
        copy.wait()
    def w_send(shard, q, to, k):
        return remote(wbuf.at[shard, q], wbuf.at[shard, q], wss.at[k], wrs.at[shard, q], v, to)

    pending = []

    def start(copy):
        copy.start()
        pending.append(copy)

    for k in range(4):
        start(w_send(b, k, right, k))
        start(w_send(b, (k + 2) % 4, left, 4 + k))
    for k in range(4):
        start(w_send(b, k, mate, 8 + k))

    mine_r = lax.rem(z - 2 * y + 8, NZ)
    mine_i = (5 * mine_r + 7) // 8
    mine_j = 5 * y + mine_i
    owner = jnp.logical_and((mine_i * 8) // 5 == mine_r, mine_j < TILES)

    load_ids.wait()
    id_row = ids[...]
    kinds = lax.broadcasted_iota(jnp.int32, (8, 256), 0)
    onehot = jnp.where(kinds == id_row, 1.0, 0.0).astype(F32)
    earlier = lax.broadcasted_iota(jnp.int32, (256, 256), 0) < lax.broadcasted_iota(
        jnp.int32, (256, 256), 1
    )
    before = jnp.dot(
        onehot.astype(BF16), jnp.where(earlier, 1.0, 0.0).astype(BF16), preferred_element_type=F32
    )
    slot_row = jnp.sum(onehot * before, axis=0, keepdims=True)
    slots = lax.broadcasted_iota(jnp.int32, (128, 256), 0).astype(F32)

    def mask_of(k):
        return jnp.logical_and(id_row == k, slot_row == slots)

    for k in range(4):
        chosen = jnp.where(mask_of(k), 1.0, 0.0)
        wide[k] = chosen
        pick[k] = chosen.astype(BF16)
    for copy in load_tok:
        copy.wait()
    load_cw.wait()
    small = jnp.zeros((4, 256), F32)
    for k in range(8):
        small += lax.dot_general(
            cw[:, 640 * k : 640 * k + 640],
            tok[k],
            (((1,), (1,)), ((), ())),
            preferred_element_type=F32,
        )
    small_top = jnp.max(small, axis=0, keepdims=True)
    rows[0:1] = small_top
    rows[1:2] = jnp.sum(jnp.exp(small - small_top), axis=0, keepdims=True)
    lane = lax.broadcasted_iota(jnp.int32, (128, 128), 1)
    before_lse = jnp.zeros((128, 128), F32)
    for k in range(4):
        logit = jnp.sum(wide[k] * small[k : k + 1], axis=1, keepdims=True)
        used = jnp.sum(wide[k], axis=1, keepdims=True)
        before_lse = jnp.where(lane == 2 + k, -logit, before_lse)
        before_lse = jnp.where(lane == 6 + k, used, before_lse)
    known[...] = before_lse
    for copy in load_out:
        copy.wait()

    def product(shard, h):
        pair = jnp.concatenate([wbuf[shard, 2 * h], wbuf[shard, 2 * h + 1]], axis=1)
        return jnp.dot(tok[shard], pair, preferred_element_type=F32)

    def head_add(shard, h):
        head_o[:, 256 * h : 256 * h + 256] += product(shard, h)

    for h in range(2):
        head_o[:, 256 * h : 256 * h + 256] = product(b, h)

    from_left = [(left, 0), (left, 1), (left, 2), (left, 3), (far, 0), (far, 1)]
    from_right = [(right, 2), (right, 3), (right, 0), (right, 1), (far, 2), (far, 3)]
    flip = 1 - 2 * c

    def w_take(s):
        for side, (shard, q) in enumerate((from_left[s], from_right[s])):
            arrived(wbuf.at[shard, q], wrs.at[shard, q])
            if s < 2:
                start(w_send(shard, q, (right, left)[side], 12 + 2 * s + side))
            start(w_send(shard, q, mate, 16 + 2 * s + side))

    def w_use(p):
        pairs = (from_left[2 * p : 2 * p + 2], from_right[2 * p : 2 * p + 2])
        for pair in pairs:
            head_add(pair[0][0], pair[0][1] // 2)
        for pair in pairs:
            for shard, q in pair:
                arrived(wbuf.at[shard + flip, q], wrs.at[shard + flip, q])
            head_add(pair[0][0] + flip, pair[0][1] // 2)

    for h in range(2):
        for q in (2 * h, 2 * h + 1):
            arrived(wbuf.at[mate, q], wrs.at[mate, q])
        head_add(mate, h)
    w_take(0)

    z_sends = [
        remote(
            pbuf.at[mine_j],
            pbuf.at[mine_j],
            pzss.at[k - 1],
            pzrs.at[mine_j],
            y * NZ + lax.rem(z + k, NZ),
            b,
        )
        for k in (4, 3, 5, 2, 6, 1, 7)
    ]

    def group_send(k):
        part = town.at[pl.ds(8 * lax.rem(y + k, NY), 8)]
        return remote(part, part, tpss.at[k], tprs.at[k], v, mate)

    first = jnp.logical_and(owner, lax.rem(mine_j, 2) == c)
    second = jnp.logical_and(owner, lax.rem(mine_j, 2) != c)

    @pl.when(first)
    def _():
        town[v] = tv[mine_j]

    @pl.when(owner)
    def _():
        total = jnp.zeros((256, 128), F32)
        for k in range(NY):
            g = lax.rem(y + k, NY)

            @pl.when(first)
            def _():
                @pl.loop(0, NZ)
                def _(s):
                    @pl.when(8 * g + s != v)
                    def _():
                        arrived(town.at[8 * g + s], trs.at[8 * g + s])

                group_send(k).start()

            @pl.when(second)
            def _():
                arrived(town.at[pl.ds(8 * g, 8)], tprs.at[k])

            for h in range(2):
                total += jnp.dot(
                    tok[2 * g + h],
                    town[pl.ds(8 * g + 4 * h, 4)].reshape(640, 128),
                    preferred_element_type=F32,
                )
        rounded = total.astype(BF16)
        low = (
            jnp.where(mine_j >= 10, 1, 0)
            + jnp.where(mine_j >= 15, 1, 0)
            + jnp.where(mine_j >= 18, 1, 0)
        )
        high = (
            jnp.where(mine_j >= 10, 1, 0)
            + jnp.where(mine_j >= 15, 1, 0)
            + jnp.where(mine_j >= 17, 1, 0)
        )
        lane = lax.broadcasted_iota(jnp.int32, (128, 128), 1)
        pbuf[mine_j] = jnp.where(
            lane < 64,
            jnp.dot(pick[low], rounded, preferred_element_type=F32),
            jnp.dot(pick[high], rounded, preferred_element_type=F32),
        ).astype(BF16)
        for copy in z_sends:
            copy.start()

    w_take(1)
    w_take(2)

    def y_send(j, i, side):
        return remote(
            pbuf.at[j],
            pbuf.at[j],
            pyss.at[i, side],
            pyrs.at[j],
            (y_up, y_down)[side] * NZ + z,
            b,
        )

    def o_send(j, i, side):
        part = pbuf.at[j, pl.ds(64 * side, 64)]
        return remote(part, part, poss.at[i, side], pors.at[j, side], (y_up, y_down)[side] * NZ + z, b)

    def relay_z(i):
        j = 5 * y + i

        @pl.when(jnp.logical_and(j < TILES, jnp.logical_not(jnp.logical_and(owner, mine_i == i))))
        def _():
            arrived(pbuf.at[j], pzrs.at[j])

        @pl.when(j < TILES)
        def _():
            for side in range(2):
                y_send(j, i, side).start()

    def relay_y(i):
        for side, ring in enumerate((y_down, y_up)):
            j = 5 * ring + i

            @pl.when(j < TILES)
            def _():
                arrived(pbuf.at[j], pyrs.at[j])
                o_send(j, i, side).start()

    def tiles(lo, hi):
        return jnp.concatenate([pbuf[t] for t in range(lo, hi)], axis=1)

    def score(ring):
        if ring < 2:
            s1_o[...] += jnp.dot(
                tiles(5 * ring, 5 * ring + 5),
                o1[640 * ring : 640 * ring + 640],
                preferred_element_type=F32,
            )
        elif ring == 2:
            s2_o[...] = jnp.dot(tiles(10, 15), o2[...], preferred_element_type=F32)
        else:
            split = pbuf[17]
            s3_o[...] = jnp.dot(
                jnp.concatenate([tiles(15, 17), split[:, :64]], axis=1),
                o3[...],
                preferred_element_type=F32,
            )
            s4_o[...] = jnp.dot(
                jnp.concatenate([split[:, 64:], pbuf[18][:, :96]], axis=1),
                o4[...],
                preferred_element_type=F32,
            )

    s1_o[...] = jnp.zeros_like(s1_o)
    for i in range(5):
        relay_z(i)
        if i == 2:
            w_use(0)
            w_take(3)
    w_use(1)
    for ring in range(NY):
        pl.when(y == ring)(lambda: score(ring))
    for i in range(5):
        relay_y(i)
        if i == 1:
            w_take(4)
        if i == 3:
            w_take(5)
    eye = lax.broadcasted_iota(jnp.int32, (128, 128), 0) == lax.broadcasted_iota(
        jnp.int32, (128, 128), 1
    )

    def as_row(col):
        return jnp.sum(jnp.where(eye, col, 0.0), axis=0, keepdims=True)

    def as_col(row):
        return jnp.sum(jnp.where(eye, row, 0.0), axis=1, keepdims=True)

    for ring in range(NY):
        pl.when(jnp.logical_or(y_up == ring, y_down == ring))(lambda: score(ring))
    w_use(2)
    head_rows = [as_row(log_sum(head_o[128 * k : 128 * k + 128])) for k in range(2)]
    for i in range(5):
        j = 5 * y_far + i

        @pl.when(j < TILES)
        def _():
            for side in range(2):
                part = pbuf.at[j, pl.ds(64 * side, 64)]
                arrived(part, pors.at[j, side])

    for ring in range(NY):
        pl.when(y_far == ring)(lambda: score(ring))
    tail_rows = [as_row(log_sum(ref[...])) for ref in (s1_o, s2_o, s3_o, s4_o)]
    packed = jnp.concatenate(head_rows + tail_rows + [jnp.zeros((2, 128), F32)], axis=0)
    msg[...] = packed
    xbuf[v] = packed

    def x_send(k):
        to = lax.rem(v + k, NV)
        return remote(msg, xbuf.at[v], xss.at[k], xrs.at[v], to, b)

    @pl.loop(1, NV)
    def _(k):
        x_send(k).start()

    for copy in pending:
        copy.wait_send()

    @pl.loop(0, TILES)
    def _(j):
        sends, copy = t_send(j)

        @pl.when(sends)
        def _():
            copy.wait_send()

    @pl.when(first)
    def _():
        for k in range(NY):
            group_send(k).wait_send()

    @pl.when(owner)
    def _():
        for copy in z_sends:
            copy.wait_send()

    for i in range(5):
        for side in range(2):

            @pl.when(5 * y + i < TILES)
            def _():
                y_send(5 * y + i, i, side).wait_send()

            j = 5 * (y_down, y_up)[side] + i

            @pl.when(j < TILES)
            def _():
                o_send(j, i, side).wait_send()

    @pl.loop(1, NV)
    def _(k):
        s = lax.rem(v + k, NV)
        arrived(xbuf.at[s], xrs.at[s])

    every = xbuf[...]
    top = jnp.max(every, axis=0)
    lse = top + jnp.log(jnp.sum(jnp.exp(every - top[None]), axis=0))
    head_lse = jnp.concatenate([lse[0:1], lse[1:2]], axis=1)
    small_top, small_sum = rows[0:1], rows[1:2]
    overall = jnp.maximum(head_lse, small_top)
    total_row = overall + jnp.log(
        jnp.exp(head_lse - overall) + small_sum * jnp.exp(small_top - overall)
    )
    found = known[...]
    for k in range(2):
        found = jnp.where(lane == k, as_col(total_row[:, 128 * k : 128 * k + 128]), found)
    for k in range(4):
        both = jnp.where(eye, lse[2 + k : 3 + k], 0.0)
        for h in range(2):
            part = slice(128 * h, 128 * h + 128)
            both += wide[k, :, part] * total_row[:, part]
        found += jnp.where(lane == 2 + k, jnp.sum(both, axis=1, keepdims=True), 0.0)
    off_o[...] = found

    @pl.loop(1, NV)
    def _(k):
        x_send(k).wait_send()


def finish(
    head_i, s1_i, s2_i, s3_i, s4_i, off_i,
    head_o, s1_o, s2_o, s3_o, s4_o,
    head_v, s1_v, s2_v, s3_v, s4_v, sems,
):
    copies = []

    def write(src, dst, sem):
        copies.append(pltpu.make_async_copy(src, dst, sem))
        copies[-1].start()

    for k in range(2):
        part = slice(128 * k, 128 * k + 128)
        head_v[part] = head_i[part] - off_i[:, k : k + 1]
        write(head_v.at[part], head_o.at[part], sems.at[k])
    tails = ((s2_i, s2_v, s2_o), (s3_i, s3_v, s3_o), (s4_i, s4_v, s4_o), (s1_i, s1_v, s1_o))
    for at, (src, held, dst) in zip((1, 2, 3, 0), tails):
        used = off_i[:, 6 + at : 7 + at] > 0.5
        held[...] = jnp.where(used, src[...] - off_i[:, 2 + at : 3 + at], 0.0)
        write(held, dst, sems.at[2 + at])
    for copy in copies:
        copy.wait()


def shards(tokens, cluster_ids, head_weight, cluster_weight, tail_proj, o1, o2, o3, o4):
    widths = [(256, 512), (128, 512), (128, 1024), (128, 1024), (128, 1024)]
    shapes = [jax.ShapeDtypeStruct(s, F32) for s in widths]
    held = [pltpu.VMEM(s, F32) for s in widths + [(128, 128)]]
    dma = pltpu.SemaphoreType.DMA
    hbm = pl.BlockSpec(memory_space=pltpu.HBM)
    vmem = pl.BlockSpec(memory_space=pltpu.VMEM)
    raw = pl.pallas_call(
        work,
        out_shape=held,
        in_specs=[hbm] * 9,
        out_specs=[vmem] * 6,
        scratch_shapes=[
            pltpu.VMEM((8, 256, 640), BF16),
            pltpu.VMEM((1, 256), jnp.int32),
            pltpu.VMEM((NB, 4, 640, 128), BF16),
            pltpu.VMEM((4, 5120), BF16),
            pltpu.VMEM((160, 2400), BF16),
            pltpu.VMEM((TILES, 2, 80, 128), BF16),
            pltpu.VMEM((NV, 2, 80, 128), BF16),
            pltpu.VMEM((TILES, 128, 128), BF16),
            pltpu.VMEM((1280, 512), BF16),
            pltpu.VMEM((640, 1024), BF16),
            pltpu.VMEM((320, 1024), BF16),
            pltpu.VMEM((160, 1024), BF16),
            pltpu.VMEM((8, 128), F32),
            pltpu.VMEM((NV, 8, 128), F32),
            pltpu.VMEM((4, 128, 256), BF16),
            pltpu.VMEM((4, 128, 256), F32),
            pltpu.VMEM((128, 128), F32),
            pltpu.VMEM((8, 256), F32),
            dma((4,)),
            dma((8,)),
            dma((7,)),
            dma((28,)),
            dma((NB, 4)),
            dma((TILES,)),
            dma((NV,)),
            dma((NY,)),
            dma((NY,)),
            dma((NZ,)),
            dma((TILES,)),
            dma((5, 2)),
            dma((TILES,)),
            dma((5, 2)),
            dma((TILES, 2)),
            dma((NV,)),
            dma((NV,)),
        ],
        compiler_params=pltpu.CompilerParams(
            collective_id=0, has_side_effects=True, vmem_limit_bytes=67043328 - 2560 * 1024
        ),
        name="work",
    )(
        tokens,
        cluster_ids.reshape(1, 256),
        head_weight,
        cluster_weight.T,
        tail_proj,
        o1,
        o2,
        o3,
        o4,
    )
    return tuple(
        pl.pallas_call(
            finish,
            out_shape=shapes,
            in_specs=[vmem] * 6,
            out_specs=[hbm] * 5,
            scratch_shapes=[pltpu.VMEM(s, F32) for s in widths] + [dma((6,))],
            compiler_params=pltpu.CompilerParams(vmem_limit_bytes=16 * 1024 * 1024),
            name="finish",
        )(*raw)
    )


def solution(mesh):
    in_specs = (
        P("batch", None),
        P("batch", None),
        P("batch", "vocab"),
        P(),
        P("vocab", None),
        P(None, "vocab"),
        P(None, "vocab"),
        P(None, "vocab"),
        P(None, "vocab"),
    )
    return jax.shard_map(
        shards, mesh=mesh, in_specs=in_specs, out_specs=(P("batch", "vocab"),) * 5, check_vma=False
    )
```
